32 devices in a mesh: dp: 8 (over z, x), cent: 4 (over y, core).
Axes of the slice: x: 2, y: 2, z: 4, core: 2. Of those that a mesh axis runs over, the one named last changes fastest.
Arguments:
- points: float32 [16384, 512], P('dp'), may hold values from -30 to 30
- centroids: float32 [16384, 512], P('cent'), may hold values from -5 to 5
Outputs:
- new_centroids: float32 [16384, 512], P('cent')
The draws below stay inside these ranges and needn't reach their ends.
All inputs are finite; a program needn't handle non-finite values.
Results may differ from the reference program's by a relative error of at most 0.0061.
Values sent between devices are 32-bit elements; how exact they have to be, the bound alone decides.
A program may use at most 128 MiB of HBM per device.

```python
import jax
import jax.numpy as jnp
from jax import lax

D = 512
K = 16384
POINTS = 16384


def shared_centroids(key):
    base = jnp.clip(jax.random.normal(jax.random.fold_in(key, 11), (K, D), jnp.float32), -5.0, 5.0)
    return base


def draw_centroids(key, part):
    return shared_centroids(key)


def draw_points(key, part):
    base = jnp.clip(jax.random.normal(jax.random.fold_in(key, 12), (POINTS, D), jnp.float32), -6.0, 6.0)
    cents = shared_centroids(key)
    picks = 2 * jax.random.randint(jax.random.fold_in(key, 15), (POINTS,), 0, K // 2)
    level = jax.random.randint(jax.random.fold_in(key, 16), (POINTS,), 0, 4).astype(jnp.float32)
    target = 110.0 + 60.0 * level
    factor = 0.5 * (target / jnp.sqrt(jnp.float32(D)) + 1.0)
    aligned = factor[:, None] * cents[picks]
    chosen = jnp.arange(POINTS) % 64 == 0
    base = jnp.where(chosen[:, None], aligned, base)
    return jnp.clip(base, -30.0, 30.0)


def setup_inputs(seed: int = 0) -> dict:
    splits = jax.random.split(jax.random.key(seed), 3)
    points = draw_points(jax.random.fold_in(splits[2], 71), 0)
    centroids = draw_centroids(jax.random.fold_in(splits[2], 71), 0)
    return {"points": points, "centroids": centroids}


def reference(points, centroids):
    cent_half = centroids.astype(jnp.bfloat16)
    sq_norm = lax.optimization_barrier(jnp.sum(centroids * centroids, axis=1))
    scale = 1.0 / jnp.sqrt(jnp.float32(D))
    block_rows = min(1024, POINTS)
    blocks = points.reshape(POINTS // block_rows, block_rows, D)

    def step(carry, block):
        weighted, counts = carry
        point_half = block.astype(jnp.bfloat16)
        inner = jnp.dot(point_half, cent_half.T, preferred_element_type=jnp.float32)
        logit = (2.0 * inner - sq_norm[None, :]) * scale
        top = lax.optimization_barrier(jnp.max(logit, axis=1, keepdims=True))
        expo = jnp.exp(logit - top)
        total = lax.optimization_barrier(jnp.sum(expo, axis=1, keepdims=True))
        resp = (expo / total).astype(jnp.bfloat16)
        weighted = weighted + jnp.dot(resp.T, point_half, preferred_element_type=jnp.float32)
        counts = counts + lax.optimization_barrier(jnp.sum(resp.astype(jnp.float32), axis=0))
        return ((weighted, counts), None)
    start = (jnp.zeros((K, D), jnp.float32), jnp.zeros((K,), jnp.float32))
    (weighted, counts), unused = lax.scan(step, start, blocks)
    return (weighted + centroids) / (counts + 1.0)[:, None]
```

```python
import functools

import jax
import jax.numpy as jnp
from jax import lax
from jax.experimental import pallas as pl
from jax.experimental.pallas import tpu as pltpu
from jax.sharding import PartitionSpec as P

MESH = pl.DeviceIdType.MESH
LANES = 128
LAG = 2
LOG2E = 1.4426950408889634


def kernel(
    ndp, ncent, geo, pts_ref, cen_ref, out_ref,
    pown, precv, ph, cenf, cenh, bias, ybuf, expo, stats, scale_ref,
    part, recv, final, cnt_part, cnt_recv, cnt_col,
    load_sem, pt_recv, px_send, py_send, pc_send, st_send, st_recv,
    rs_send, rs_recv, cn_send, cn_recv, ag_send, ag_recv, xp_send, xp_recv, out_sem,
):
    rows, half, pb, sub, kb, mb, chunk = geo
    width = pts_ref.shape[1]
    chain = ndp // 2
    last = chain - 1
    dirs = half // 2
    count = dirs // chunk
    share = rows // ncent
    nsub = share // sub
    nblk = share // pb
    per = pb // sub
    nrow = 2 * rows // LANES

    me = lax.axis_index("dp")
    cent = lax.axis_index("cent")
    z, x = me // 2, lax.rem(me, 2)
    core, yy = lax.rem(cent, 2), cent // 2
    other = z * 2 + (1 - x)
    mate = yy * 2 + (1 - core)
    mine = x * ncent + cent

    def remote(src, dst, send, got, dp, ce):
        return pltpu.make_async_remote_copy(
            src_ref=src, dst_ref=dst, send_sem=send, recv_sem=got,
            device_id=(dp, ce), device_id_type=MESH,
        )

    load_p = pltpu.make_async_copy(pts_ref, pown, load_sem.at[0])
    load_c = pltpu.make_async_copy(
        cen_ref.at[pl.ds(pl.multiple_of(x * half, half), half)], cenf, load_sem.at[1]
    )
    load_p.start()
    load_c.start()
    load_p.wait()

    def span(owner, j):
        return pl.ds(pl.multiple_of(owner * share + j * sub, sub), sub)

    swaps = []
    for j in range(nsub):
        copy = remote(
            pown.at[span(cent, j)], precv.at[span(cent, j)],
            px_send.at[j], pt_recv.at[cent * nsub + j], other, cent,
        )
        copy.start()
        swaps.append(copy)
    load_c.wait()

    root = jnp.float32(1.0) / jnp.sqrt(jnp.float32(width))
    gain = 2.0 * root * LOG2E
    norm_gain = root * LOG2E

    def prepare(k, carry):
        at = pl.ds(pl.multiple_of(k * mb, mb), mb)
        c = cenf[at, :]
        cenh[at, :] = c.astype(jnp.bfloat16)
        bias[at, :] = jnp.broadcast_to(
            jnp.sum(c * c, axis=1, keepdims=True) * norm_gain, (mb, LANES)
        )
        return carry

    lax.fori_loop(0, half // mb, prepare, 0)

    def block(src, row, col):
        pv = src[pl.ds(pl.multiple_of(row, pb), pb), :].astype(jnp.bfloat16)
        cols = pl.ds(pl.multiple_of(col, pb), pb)
        ph[cols, :] = pv

        def logits(k, top):
            at = pl.ds(pl.multiple_of(k * kb, kb), kb)
            inner = lax.dot_general(
                cenh[at, :], pv, (((1,), (1,)), ((), ())), preferred_element_type=jnp.float32
            )
            b = bias[at, :]
            y = inner * gain - jnp.concatenate([b] * (pb // LANES), axis=1)
            ybuf[at, :] = y
            return jnp.maximum(top, jnp.max(y, axis=0, keepdims=True))

        top = lax.fori_loop(
            0, half // kb, logits, jnp.full((1, pb), -jnp.inf, jnp.float32)
        )

        def powers(k, total):
            at = pl.ds(pl.multiple_of(k * kb, kb), kb)
            e = jnp.exp2(ybuf[at, :] - top)
            expo[at, cols] = e.astype(jnp.bfloat16)
            return total + jnp.sum(e, axis=0, keepdims=True)

        total = lax.fori_loop(0, half // kb, powers, jnp.zeros((1, pb), jnp.float32))
        base = col // LANES
        for h in range(pb // LANES):
            stats[mine, pl.ds(base + h, 1), :] = top[:, h * LANES:(h + 1) * LANES]
            stats[mine, pl.ds(nrow + base + h, 1), :] = total[:, h * LANES:(h + 1) * LANES]

    def own(b, carry):
        block(pown, b * pb, x * rows + b * pb)
        return carry

    lax.fori_loop(0, rows // pb, own, 0)

    sends = []

    def arrived(owner, j):
        remote(
            precv.at[span(owner, j)], precv.at[span(owner, j)],
            px_send.at[0], pt_recv.at[owner * nsub + j], other, cent,
        ).wait_recv()

    def forward(owner, j, dp, ce, sem):
        copy = remote(
            precv.at[span(owner, j)], precv.at[span(owner, j)],
            sem, pt_recv.at[owner * nsub + j], dp, ce,
        )
        copy.start()
        sends.append(copy)

    ny = ncent // 2
    same = [lax.rem(yy + d, ny) * 2 + core for d in range(1, ny)]
    cross = [lax.rem(yy + d, ny) * 2 + (1 - core) for d in range(1, ny)]

    def theirs(owner, b, wait):
        if wait:
            for j in range(per):
                arrived(owner, b * per + j)
        row = owner * share + b * pb
        block(precv, row, (1 - x) * rows + row)

    for j in range(nsub + 1):
        if j < nsub:
            arrived(cent, j)
            for i, d in enumerate(same):
                forward(cent, j, me, d, py_send.at[i * nsub + j])
            forward(cent, j, me, mate, pc_send.at[j])
        if j >= 1:
            for i, d in enumerate(same):
                arrived(d, j - 1)
                forward(d, j - 1, me, mate, pc_send.at[(i + 1) * nsub + j - 1])
        if j < nsub and j % per == per - 1:
            theirs(cent, j // per, False)
        if j >= 1 and (j - 1) % per == per - 1:
            theirs(mate, (j - 1) // per, True)
    for b in range(nblk):
        for d in same:
            theirs(d, b, False)
        for d in cross:
            theirs(d, b, True)

    group = 2 * ncent
    stat_sends = []
    for o in range(1, group):
        peer = lax.rem(mine + o, group)
        copy = remote(
            stats.at[mine], stats.at[mine], st_send.at[o], st_recv.at[mine],
            z * 2 + peer // ncent, lax.rem(peer, ncent),
        )
        copy.start()
        stat_sends.append(copy)
    for o in range(1, group):
        peer = lax.rem(mine + o, group)
        remote(
            stats.at[peer], stats.at[peer], st_send.at[o], st_recv.at[peer], other, cent
        ).wait_recv()
    high = stats[0, 0:nrow, :]
    for s in range(1, group):
        high = jnp.maximum(high, stats[s, 0:nrow, :])
    summed = jnp.zeros((nrow, LANES), jnp.float32)
    for s in range(group):
        summed = summed + stats[s, nrow:, :] * jnp.exp2(stats[s, 0:nrow, :] - high)
    scale_ref[...] = jnp.exp2(stats[mine, 0:nrow, :] - high) / summed

    def place(d):
        return z if d == 0 else last - z

    def ahead(d):
        return (z + 1 if d == 0 else z - 1) * 2 + x

    def behind(d):
        return (z - 1 if d == 0 else z + 1) * 2 + x

    def crows(d, i):
        return pl.ds(pl.multiple_of(d * dirs + i * chunk, chunk), chunk)

    pair = LANES // chunk
    ncnt = count // pair

    def pass_on(d, i, src, cnt):
        remote(
            src.at[crows(d, i)], recv.at[crows(d, i)],
            rs_send.at[d], rs_recv.at[d * count + i], ahead(d), cent,
        ).start()

        @pl.when(lax.rem(i, pair) == 0)
        def _():
            slot = d * ncnt + i // pair
            remote(
                cnt.at[slot], cnt_recv.at[slot], cn_send.at[d], cn_recv.at[slot], ahead(d), cent
            ).start()

    def weigh(d, j):
        at = pl.ds(pl.multiple_of(d * dirs + j * mb, mb), mb)

        def rescale(q, acc):
            cols = pl.ds(pl.multiple_of(q * LANES, LANES), LANES)
            r = expo[at, cols].astype(jnp.float32) * scale_ref[pl.ds(q, 1), :]
            r = r.astype(jnp.bfloat16)
            expo[at, cols] = r
            return acc + r.astype(jnp.float32)

        acc = lax.fori_loop(0, nrow, rescale, jnp.zeros((mb, LANES), jnp.float32), unroll=2)
        for h in range(mb // LANES):
            line = jnp.sum(acc[h * LANES:(h + 1) * LANES, :].T, axis=0, keepdims=True)
            cnt_part[d * ncnt + j * (mb // LANES) + h] = jnp.broadcast_to(line, (8, LANES))
        part[at, :] = jnp.dot(expo[at, :], ph[...], preferred_element_type=jnp.float32)

        for which in (0, 1):
            @pl.when(jnp.logical_and(d == which, place(which) == 0))
            def _():
                for i in range(mb // chunk):
                    pass_on(which, j * (mb // chunk) + i, part, cnt_part)

    def both(t, carry):
        first = jnp.where(z < chain // 2, 0, 1)
        d = lax.rem(first + lax.rem(t, 2), 2)
        weigh(d, t // 2)
        return carry

    lax.fori_loop(0, 2 * (dirs // mb), both, 0)

    def hand_out(d, i):
        rows_out = pl.ds(pl.multiple_of(x * half + d * dirs + i * chunk, chunk), chunk)
        src = final.at[crows(d, i)]
        remote(src, out_ref.at[rows_out], xp_send.at[d], xp_recv.at[d], other, cent).start()
        pltpu.make_async_copy(src, out_ref.at[rows_out], out_sem.at[d]).start()

        @pl.when(place(d) > 0)
        def _():
            remote(
                src, src, ag_send.at[d], ag_recv.at[d * count + i], behind(d), cent
            ).start()

    def tick(t, carry):
        for d in (0, 1):
            pos = place(d)
            i = t - LAG * pos

            @pl.when((pos > 0) & (i >= 0) & (i < count))
            def _():
                at = crows(d, i)
                slot = d * ncnt + i // pair
                remote(
                    recv.at[at], recv.at[at], rs_send.at[d], rs_recv.at[d * count + i], other, cent
                ).wait_recv()

                @pl.when(lax.rem(i, pair) == 0)
                def _():
                    remote(
                        cnt_recv.at[slot], cnt_recv.at[slot],
                        cn_send.at[d], cn_recv.at[slot], other, cent,
                    ).wait_recv()

                @pl.when(pos < last)
                def _():
                    recv[at, :] = recv[at, :] + part[at, :]

                    @pl.when(lax.rem(i, pair) == 0)
                    def _():
                        cnt_recv[slot] = cnt_recv[slot] + cnt_part[slot]

                    pass_on(d, i, recv, cnt_recv)

                @pl.when(pos == last)
                def _():
                    @pl.when(lax.rem(i, pair) == 0)
                    def _():
                        line = cnt_recv[slot] + cnt_part[slot] + 1.0
                        cnt_col[d] = jnp.broadcast_to(line[0:1, :], (LANES, LANES)).T

                    div = cnt_col[d, pl.ds(pl.multiple_of(lax.rem(i, pair) * chunk, chunk), chunk), :]
                    div = jnp.concatenate([div] * (width // LANES), axis=1)
                    final[at, :] = (recv[at, :] + part[at, :] + cenf[at, :]) / div
                    hand_out(d, i)

        for d in (0, 1):
            pos = place(d)
            i = t - LAG * (2 * last - pos)

            @pl.when((pos < last) & (i >= 0) & (i < count))
            def _():
                at = crows(d, i)
                remote(
                    final.at[at], final.at[at], ag_send.at[d], ag_recv.at[d * count + i], other, cent
                ).wait_recv()
                hand_out(d, i)

        return carry

    lax.fori_loop(0, count + LAG * 2 * last, tick, 0)

    for copy in swaps + sends + stat_sends:
        copy.wait_send()
    for d in (0, 1):
        at = pl.ds(d * dirs, dirs)
        cs = pl.ds(d * ncnt, ncnt)

        @pl.when(place(d) < last)
        def _():
            remote(recv.at[at], recv.at[at], rs_send.at[d], rs_recv.at[0], other, cent).wait_send()
            remote(
                cnt_recv.at[cs], cnt_recv.at[cs], cn_send.at[d], cn_recv.at[0], other, cent
            ).wait_send()

        @pl.when(place(d) > 0)
        def _():
            remote(final.at[at], final.at[at], ag_send.at[d], ag_recv.at[0], other, cent).wait_send()

        here = pl.ds(pl.multiple_of(x * half + d * dirs, dirs), dirs)
        there = pl.ds(pl.multiple_of((1 - x) * half + d * dirs, dirs), dirs)
        pltpu.make_async_copy(final.at[at], out_ref.at[here], out_sem.at[d]).wait()
        remote(final.at[at], out_ref.at[there], xp_send.at[d], xp_recv.at[d], other, cent).wait()


def body(ndp, ncent, points, centroids):
    rows, width = points.shape
    half = centroids.shape[0] // 2
    share = rows // ncent
    pb = min(256, share)
    sub = pb // 2
    kb, mb, chunk = 512, 256, 64
    dirs = half // 2
    count = dirs // chunk
    ncnt = dirs // LANES
    nsub = share // sub
    ny = ncent // 2
    nrow = 2 * rows // LANES
    f32, bf16 = jnp.float32, jnp.bfloat16
    dma = pltpu.SemaphoreType.DMA
    return pl.pallas_call(
        functools.partial(kernel, ndp, ncent, (rows, half, pb, sub, kb, mb, chunk)),
        out_shape=jax.ShapeDtypeStruct(centroids.shape, f32),
        in_specs=[pl.BlockSpec(memory_space=pl.ANY)] * 2,
        out_specs=pl.BlockSpec(memory_space=pl.ANY),
        scratch_shapes=[
            pltpu.VMEM((rows, width), f32),
            pltpu.VMEM((rows, width), f32),
            pltpu.VMEM((2 * rows, width), bf16),
            pltpu.VMEM((half, width), f32),
            pltpu.VMEM((half, width), bf16),
            pltpu.VMEM((half, LANES), f32),
            pltpu.VMEM((half, pb), f32),
            pltpu.VMEM((half, 2 * rows), bf16),
            pltpu.VMEM((2 * ncent, 2 * nrow, LANES), f32),
            pltpu.VMEM((nrow, LANES), f32),
            pltpu.VMEM((half, width), f32),
            pltpu.VMEM((half, width), f32),
            pltpu.VMEM((half, width), f32),
            pltpu.VMEM((2 * ncnt, 8, LANES), f32),
            pltpu.VMEM((2 * ncnt, 8, LANES), f32),
            pltpu.VMEM((2, LANES, LANES), f32),
            dma((2,)),
            dma((ncent * nsub,)),
            dma((nsub,)),
            dma(((ny - 1) * nsub,)),
            dma((ny * nsub,)),
            dma((2 * ncent,)),
            dma((2 * ncent,)),
            dma((2,)),
            dma((2 * count,)),
            dma((2,)),
            dma((2 * ncnt,)),
            dma((2,)),
            dma((2 * count,)),
            dma((2,)),
            dma((2,)),
            dma((2,)),
        ],
        compiler_params=pltpu.CompilerParams(
            has_side_effects=True, vmem_limit_bytes=63 * 2**20
        ),
        name="kmeans",
    )(points, centroids)


def solution(mesh):
    placed = (P("dp", None), P("cent", None))
    return jax.shard_map(
        functools.partial(body, mesh.shape["dp"], mesh.shape["cent"]),
        mesh=mesh, in_specs=placed, out_specs=P("cent", None), check_vma=False,
    )
```

```python
import functools

import jax
import jax.numpy as jnp
from jax import lax
from jax.experimental import pallas as pl
from jax.experimental.pallas import tpu as pltpu
from jax.sharding import PartitionSpec as P

MESH = pl.DeviceIdType.MESH
LANES = 128
LAG = 2
LOG2E = 1.4426950408889634


def kernel(
    ndp, ncent, geo, pts_ref, cen_ref, out_ref,
    pown, precv, ph, cenf, cenh, bias, ybuf, expo, stats, scale_ref,
    part, recv, final, cnt_part, cnt_recv, cnt_col,
    load_sem, pt_recv, px_send, py_send, pc_send, st_send, st_recv,
    rs_send, rs_recv, cn_send, cn_recv, ag_send, ag_recv, xp_send, xp_recv, out_sem,
):
    rows, half, pb, sub, kb, mb, chunk = geo
    width = pts_ref.shape[1]
    chain = ndp // 2
    last = chain - 1
    dirs = half // 2
    count = dirs // chunk
    share = rows // ncent
    nsub = share // sub
    nblk = share // pb
    per = pb // sub
    nrow = 2 * rows // LANES

    me = lax.axis_index("dp")
    cent = lax.axis_index("cent")
    z, x = me // 2, lax.rem(me, 2)
    core, yy = lax.rem(cent, 2), cent // 2
    other = z * 2 + (1 - x)
    mate = yy * 2 + (1 - core)
    mine = x * ncent + cent

    def remote(src, dst, send, got, dp, ce):
        return pltpu.make_async_remote_copy(
            src_ref=src, dst_ref=dst, send_sem=send, recv_sem=got,
            device_id=(dp, ce), device_id_type=MESH,
        )

    load_p = pltpu.make_async_copy(pts_ref, pown, load_sem.at[0])
    load_c = pltpu.make_async_copy(
        cen_ref.at[pl.ds(pl.multiple_of(x * half, half), half)], cenf, load_sem.at[1]
    )
    load_p.start()
    load_c.start()

    barrier = pltpu.get_barrier_semaphore()
    for o in range(1, 2 * ncent):
        peer = lax.rem(mine + o, 2 * ncent)
        pl.semaphore_signal(
            barrier, inc=1, device_id=(z * 2 + peer // ncent, lax.rem(peer, ncent)),
            device_id_type=MESH,
        )

    @pl.when(z > 0)
    def _():
        pl.semaphore_signal(barrier, inc=1, device_id=(me - 2, cent), device_id_type=MESH)

    @pl.when(z < last)
    def _():
        pl.semaphore_signal(barrier, inc=1, device_id=(me + 2, cent), device_id_type=MESH)

    ends = jnp.where(z > 0, 1, 0) + jnp.where(z < last, 1, 0)
    pl.semaphore_wait(barrier, 2 * ncent - 1 + ends)
    load_p.wait()

    def span(owner, j):
        return pl.ds(pl.multiple_of(owner * share + j * sub, sub), sub)

    swaps = []
    for j in range(nsub):
        copy = remote(
            pown.at[span(cent, j)], precv.at[span(cent, j)],
            px_send.at[j], pt_recv.at[cent * nsub + j], other, cent,
        )
        copy.start()
        swaps.append(copy)
    load_c.wait()

    root = jnp.float32(1.0) / jnp.sqrt(jnp.float32(width))
    gain = 2.0 * root * LOG2E
    norm_gain = root * LOG2E

    def prepare(k, carry):
        at = pl.ds(pl.multiple_of(k * mb, mb), mb)
        c = cenf[at, :]
        cenh[at, :] = c.astype(jnp.bfloat16)
        bias[at, :] = jnp.broadcast_to(
            jnp.sum(c * c, axis=1, keepdims=True) * norm_gain, (mb, LANES)
        )
        return carry

    lax.fori_loop(0, half // mb, prepare, 0)

    def block(src, row, col):
        pv = src[pl.ds(pl.multiple_of(row, pb), pb), :].astype(jnp.bfloat16)
        cols = pl.ds(pl.multiple_of(col, pb), pb)
        ph[cols, :] = pv

        def logits(k, top):
            at = pl.ds(pl.multiple_of(k * kb, kb), kb)
            inner = lax.dot_general(
                cenh[at, :], pv, (((1,), (1,)), ((), ())), preferred_element_type=jnp.float32
            )
            b = bias[at, :]
            y = inner * gain - jnp.concatenate([b] * (pb // LANES), axis=1)
            ybuf[at, :] = y
            return jnp.maximum(top, jnp.max(y, axis=0, keepdims=True))

        top = lax.fori_loop(
            0, half // kb, logits, jnp.full((1, pb), -jnp.inf, jnp.float32), unroll=True
        )

        def powers(k, total):
            at = pl.ds(pl.multiple_of(k * kb, kb), kb)
            e = jnp.exp2(ybuf[at, :] - top)
            expo[at, cols] = e.astype(jnp.bfloat16)
            return total + jnp.sum(e, axis=0, keepdims=True)

        total = lax.fori_loop(0, half // kb, powers, jnp.zeros((1, pb), jnp.float32), unroll=True)
        base = col // LANES
        for h in range(pb // LANES):
            stats[mine, pl.ds(base + h, 1), :] = top[:, h * LANES:(h + 1) * LANES]
            stats[mine, pl.ds(nrow + base + h, 1), :] = total[:, h * LANES:(h + 1) * LANES]

    def own(b, carry):
        block(pown, b * pb, x * rows + b * pb)
        return carry

    sends = []

    def arrived(owner, j):
        remote(
            precv.at[span(owner, j)], precv.at[span(owner, j)],
            px_send.at[0], pt_recv.at[owner * nsub + j], other, cent,
        ).wait_recv()

    def forward(owner, j, dp, ce, sem):
        copy = remote(
            precv.at[span(owner, j)], precv.at[span(owner, j)],
            sem, pt_recv.at[owner * nsub + j], dp, ce,
        )
        copy.start()
        sends.append(copy)

    ny = ncent // 2
    same = [lax.rem(yy + d, ny) * 2 + core for d in range(1, ny)]
    cross = [lax.rem(yy + d, ny) * 2 + (1 - core) for d in range(1, ny)]

    def theirs(owner, b, wait):
        if wait:
            for j in range(per):
                arrived(owner, b * per + j)
        row = owner * share + b * pb
        block(precv, row, (1 - x) * rows + row)

    nown = rows // pb
    lax.fori_loop(0, nown // 2, own, 0)
    for j in range(nsub + 1):
        if j == 1:
            lax.fori_loop(nown // 2, nown, own, 0)
        if j < nsub:
            arrived(cent, j)
            for i, d in enumerate(same):
                forward(cent, j, me, d, py_send.at[i * nsub + j])
            forward(cent, j, me, mate, pc_send.at[j])
        if j >= 1:
            for i, d in enumerate(same):
                arrived(d, j - 1)
                forward(d, j - 1, me, mate, pc_send.at[(i + 1) * nsub + j - 1])
        if j < nsub and j % per == per - 1:
            theirs(cent, j // per, False)
        if j >= 1 and (j - 1) % per == per - 1:
            theirs(mate, (j - 1) // per, True)
    for b in range(nblk):
        for d in same:
            theirs(d, b, False)
        for d in cross:
            theirs(d, b, True)

    group = 2 * ncent
    stat_sends = []
    for o in range(1, group):
        peer = lax.rem(mine + o, group)
        copy = remote(
            stats.at[mine], stats.at[mine], st_send.at[o], st_recv.at[mine],
            z * 2 + peer // ncent, lax.rem(peer, ncent),
        )
        copy.start()
        stat_sends.append(copy)
    for o in range(1, group):
        peer = lax.rem(mine + o, group)
        remote(
            stats.at[peer], stats.at[peer], st_send.at[o], st_recv.at[peer], other, cent
        ).wait_recv()
    high = stats[0, 0:nrow, :]
    for s in range(1, group):
        high = jnp.maximum(high, stats[s, 0:nrow, :])
    summed = jnp.zeros((nrow, LANES), jnp.float32)
    for s in range(group):
        summed = summed + stats[s, nrow:, :] * jnp.exp2(stats[s, 0:nrow, :] - high)
    scale_ref[...] = jnp.exp2(stats[mine, 0:nrow, :] - high) / summed

    def place(d):
        return z if d == 0 else last - z

    def ahead(d):
        return (z + 1 if d == 0 else z - 1) * 2 + x

    def behind(d):
        return (z - 1 if d == 0 else z + 1) * 2 + x

    def crows(d, i):
        return pl.ds(pl.multiple_of(d * dirs + i * chunk, chunk), chunk)

    pair = LANES // chunk
    ncnt = count // pair
    window = LAG * last

    def pass_on(d, i, src, cnt):
        remote(
            src.at[crows(d, i)], recv.at[crows(d, i)],
            rs_send.at[d], rs_recv.at[d * count + i], ahead(d), cent,
        ).start()

        @pl.when(lax.rem(i, pair) == 0)
        def _():
            slot = d * ncnt + i // pair
            remote(
                cnt.at[slot], cnt_recv.at[slot], cn_send.at[d], cn_recv.at[slot], ahead(d), cent
            ).start()

    def weigh(d, j):
        at = pl.ds(pl.multiple_of(d * dirs + j * mb, mb), mb)

        def rescale(q, acc):
            cols = pl.ds(pl.multiple_of(q * LANES, LANES), LANES)
            r = expo[at, cols].astype(jnp.float32) * scale_ref[pl.ds(q, 1), :]
            r = r.astype(jnp.bfloat16)
            expo[at, cols] = r
            return acc + r.astype(jnp.float32)

        acc = lax.fori_loop(0, nrow, rescale, jnp.zeros((mb, LANES), jnp.float32), unroll=2)
        for h in range(mb // LANES):
            line = jnp.sum(acc[h * LANES:(h + 1) * LANES, :].T, axis=0, keepdims=True)
            cnt_part[d * ncnt + j * (mb // LANES) + h] = jnp.broadcast_to(line, (8, LANES))
        part[at, :] = jnp.dot(expo[at, :], ph[...], preferred_element_type=jnp.float32)

        for which in (0, 1):
            @pl.when(jnp.logical_and(d == which, place(which) == 0))
            def _():
                for h in range(mb // chunk):
                    i = j * (mb // chunk) + h

                    @pl.when(i < window)
                    def _():
                        pass_on(which, i, part, cnt_part)

    def both(t, carry):
        first = jnp.where(z < chain // 2, 0, 1)
        d = lax.rem(first + lax.rem(t, 2), 2)
        weigh(d, t // 2)
        return carry

    def hand_out(d, i):
        rows_out = pl.ds(pl.multiple_of(x * half + d * dirs + i * chunk, chunk), chunk)
        src = final.at[crows(d, i)]
        remote(src, out_ref.at[rows_out], xp_send.at[d], xp_recv.at[d], other, cent).start()
        pltpu.make_async_copy(src, out_ref.at[rows_out], out_sem.at[d]).start()

        @pl.when(place(d) > 0)
        def _():
            remote(
                src, src, ag_send.at[d], ag_recv.at[d * count + i], behind(d), cent
            ).start()

    def tick(t, carry):
        for d in (0, 1):
            pos = place(d)
            i = t - LAG * pos

            @pl.when((pos == 0) & (i >= window) & (i < count))
            def _():
                pass_on(d, i, part, cnt_part)

            @pl.when((pos > 0) & (i >= 0) & (i < count))
            def _():
                at = crows(d, i)
                slot = d * ncnt + i // pair
                remote(
                    recv.at[at], recv.at[at], rs_send.at[d], rs_recv.at[d * count + i], other, cent
                ).wait_recv()

                @pl.when(lax.rem(i, pair) == 0)
                def _():
                    remote(
                        cnt_recv.at[slot], cnt_recv.at[slot],
                        cn_send.at[d], cn_recv.at[slot], other, cent,
                    ).wait_recv()

                @pl.when(pos < last)
                def _():
                    recv[at, :] = recv[at, :] + part[at, :]

                    @pl.when(lax.rem(i, pair) == 0)
                    def _():
                        cnt_recv[slot] = cnt_recv[slot] + cnt_part[slot]

                    pass_on(d, i, recv, cnt_recv)

                @pl.when(pos == last)
                def _():
                    @pl.when(lax.rem(i, pair) == 0)
                    def _():
                        line = cnt_recv[slot] + cnt_part[slot] + 1.0
                        cnt_col[d] = jnp.broadcast_to(line[0:1, :], (LANES, LANES)).T

                    div = cnt_col[d, pl.ds(pl.multiple_of(lax.rem(i, pair) * chunk, chunk), chunk), :]
                    div = jnp.concatenate([div] * (width // LANES), axis=1)
                    final[at, :] = (recv[at, :] + part[at, :] + cenf[at, :]) / div
                    hand_out(d, i)

        for d in (0, 1):
            pos = place(d)
            i = t - LAG * (2 * last - pos)

            @pl.when((pos < last) & (i >= 0) & (i < count))
            def _():
                at = crows(d, i)
                remote(
                    final.at[at], final.at[at], ag_send.at[d], ag_recv.at[d * count + i], other, cent
                ).wait_recv()
                hand_out(d, i)

        return carry

    units = 2 * (dirs // mb)
    early = max(2, units - window)

    def mixed(t, carry):
        tick(t, carry)
        return both(early + t, carry)

    lax.fori_loop(0, early, both, 0)
    lax.fori_loop(0, units - early, mixed, 0)
    lax.fori_loop(units - early, count + LAG * 2 * last, tick, 0)

    for copy in swaps + sends + stat_sends:
        copy.wait_send()
    for d in (0, 1):
        at = pl.ds(d * dirs, dirs)
        cs = pl.ds(d * ncnt, ncnt)

        @pl.when(place(d) < last)
        def _():
            remote(recv.at[at], recv.at[at], rs_send.at[d], rs_recv.at[0], other, cent).wait_send()
            remote(
                cnt_recv.at[cs], cnt_recv.at[cs], cn_send.at[d], cn_recv.at[0], other, cent
            ).wait_send()

        @pl.when(place(d) > 0)
        def _():
            remote(final.at[at], final.at[at], ag_send.at[d], ag_recv.at[0], other, cent).wait_send()

        here = pl.ds(pl.multiple_of(x * half + d * dirs, dirs), dirs)
        there = pl.ds(pl.multiple_of((1 - x) * half + d * dirs, dirs), dirs)
        pltpu.make_async_copy(final.at[at], out_ref.at[here], out_sem.at[d]).wait()
        remote(final.at[at], out_ref.at[there], xp_send.at[d], xp_recv.at[d], other, cent).wait()


def body(ndp, ncent, points, centroids):
    rows, width = points.shape
    half = centroids.shape[0] // 2
    share = rows // ncent
    pb = min(256, share)
    sub = pb // 4
    kb, mb, chunk = 512, 256, 32
    dirs = half // 2
    count = dirs // chunk
    ncnt = dirs // LANES
    nsub = share // sub
    ny = ncent // 2
    nrow = 2 * rows // LANES
    f32, bf16 = jnp.float32, jnp.bfloat16
    dma = pltpu.SemaphoreType.DMA
    return pl.pallas_call(
        functools.partial(kernel, ndp, ncent, (rows, half, pb, sub, kb, mb, chunk)),
        out_shape=jax.ShapeDtypeStruct(centroids.shape, f32),
        in_specs=[pl.BlockSpec(memory_space=pl.ANY)] * 2,
        out_specs=pl.BlockSpec(memory_space=pl.ANY),
        scratch_shapes=[
            pltpu.VMEM((rows, width), f32),
            pltpu.VMEM((rows, width), f32),
            pltpu.VMEM((2 * rows, width), bf16),
            pltpu.VMEM((half, width), f32),
            pltpu.VMEM((half, width), bf16),
            pltpu.VMEM((half, LANES), f32),
            pltpu.VMEM((half, pb), f32),
            pltpu.VMEM((half, 2 * rows), bf16),
            pltpu.VMEM((2 * ncent, 2 * nrow, LANES), f32),
            pltpu.VMEM((nrow, LANES), f32),
            pltpu.VMEM((half, width), f32),
            pltpu.VMEM((half, width), f32),
            pltpu.VMEM((half, width), f32),
            pltpu.VMEM((2 * ncnt, 8, LANES), f32),
            pltpu.VMEM((2 * ncnt, 8, LANES), f32),
            pltpu.VMEM((2, LANES, LANES), f32),
            dma((2,)),
            dma((ncent * nsub,)),
            dma((nsub,)),
            dma(((ny - 1) * nsub,)),
            dma((ny * nsub,)),
            dma((2 * ncent,)),
            dma((2 * ncent,)),
            dma((2,)),
            dma((2 * count,)),
            dma((2,)),
            dma((2 * ncnt,)),
            dma((2,)),
            dma((2 * count,)),
            dma((2,)),
            dma((2,)),
            dma((2,)),
        ],
        compiler_params=pltpu.CompilerParams(
            collective_id=0, has_side_effects=True, vmem_limit_bytes=63 * 2**20
        ),
        name="kmeans",
    )(points, centroids)


def solution(mesh):
    placed = (P("dp", None), P("cent", None))
    return jax.shard_map(
        functools.partial(body, mesh.shape["dp"], mesh.shape["cent"]),
        mesh=mesh, in_specs=placed, out_specs=P("cent", None), check_vma=False,
    )
```

```python
import functools

import jax
import jax.numpy as jnp
from jax import lax
from jax.experimental import pallas as pl
from jax.experimental.pallas import tpu as pltpu
from jax.sharding import PartitionSpec as P

MESH = pl.DeviceIdType.MESH
LANES = 128
LAG = 2
LOG2E = 1.4426950408889634


def kernel(
    ndp, ncent, geo, pts_ref, cen_ref, out_ref,
    pown, precv, ph, cenf, cenh, bias, ybuf, expo, stats, scale_ref,
    part, recv, final, cnt_part, cnt_recv, cnt_col,
    load_sem, pt_recv, px_send, py_send, pc_send, st_send, st_recv,
    rs_send, rs_recv, cn_send, cn_recv, ag_send, ag_recv, xp_send, xp_recv, out_sem,
):
    rows, half, pb, sub, kb, mb, chunk = geo
    width = pts_ref.shape[1]
    chain = ndp // 2
    last = chain - 1
    dirs = half // 2
    count = dirs // chunk
    share = rows // ncent
    nsub = share // sub
    nblk = share // pb
    per = pb // sub
    nrow = 2 * rows // LANES

    me = lax.axis_index("dp")
    cent = lax.axis_index("cent")
    z, x = me // 2, lax.rem(me, 2)
    core, yy = lax.rem(cent, 2), cent // 2
    other = z * 2 + (1 - x)
    mate = yy * 2 + (1 - core)
    mine = x * ncent + cent

    def remote(src, dst, send, got, dp, ce):
        return pltpu.make_async_remote_copy(
            src_ref=src, dst_ref=dst, send_sem=send, recv_sem=got,
            device_id=(dp, ce), device_id_type=MESH,
        )

    load_p = pltpu.make_async_copy(pts_ref, pown, load_sem.at[0])
    load_c = pltpu.make_async_copy(
        cen_ref.at[pl.ds(pl.multiple_of(x * half, half), half)], cenf, load_sem.at[1]
    )
    load_p.start()
    load_c.start()

    barrier = pltpu.get_barrier_semaphore()
    for o in range(1, 2 * ncent):
        peer = lax.rem(mine + o, 2 * ncent)
        pl.semaphore_signal(
            barrier, inc=1, device_id=(z * 2 + peer // ncent, lax.rem(peer, ncent)),
            device_id_type=MESH,
        )

    @pl.when(z > 0)
    def _():
        pl.semaphore_signal(barrier, inc=1, device_id=(me - 2, cent), device_id_type=MESH)

    @pl.when(z < last)
    def _():
        pl.semaphore_signal(barrier, inc=1, device_id=(me + 2, cent), device_id_type=MESH)

    ends = jnp.where(z > 0, 1, 0) + jnp.where(z < last, 1, 0)
    pl.semaphore_wait(barrier, 2 * ncent - 1 + ends)
    load_p.wait()

    def span(owner, j):
        return pl.ds(pl.multiple_of(owner * share + j * sub, sub), sub)

    swaps = []
    for j in range(nsub):
        copy = remote(
            pown.at[span(cent, j)], precv.at[span(cent, j)],
            px_send.at[j], pt_recv.at[cent * nsub + j], other, cent,
        )
        copy.start()
        swaps.append(copy)
    load_c.wait()

    root = jnp.float32(1.0) / jnp.sqrt(jnp.float32(width))
    gain = 2.0 * root * LOG2E
    norm_gain = root * LOG2E

    def prepare(k, carry):
        at = pl.ds(pl.multiple_of(k * mb, mb), mb)
        c = cenf[at, :]
        cenh[at, :] = c.astype(jnp.bfloat16)
        bias[at, :] = jnp.broadcast_to(
            jnp.sum(c * c, axis=1, keepdims=True) * norm_gain, (mb, LANES)
        )
        return carry

    lax.fori_loop(0, half // mb, prepare, 0)

    def block(src, row, col):
        pv = src[pl.ds(pl.multiple_of(row, pb), pb), :].astype(jnp.bfloat16)
        cols = pl.ds(pl.multiple_of(col, pb), pb)
        ph[cols, :] = pv

        def logits(k, top):
            at = pl.ds(pl.multiple_of(k * kb, kb), kb)
            inner = lax.dot_general(
                cenh[at, :], pv, (((1,), (1,)), ((), ())), preferred_element_type=jnp.float32
            )
            b = bias[at, :]
            y = inner * gain - jnp.concatenate([b] * (pb // LANES), axis=1)
            ybuf[at, :] = y
            return jnp.maximum(top, jnp.max(y, axis=0, keepdims=True))

        top = lax.fori_loop(
            0, half // kb, logits, jnp.full((1, pb), -jnp.inf, jnp.float32), unroll=True
        )

        def powers(k, total):
            at = pl.ds(pl.multiple_of(k * kb, kb), kb)
            e = jnp.exp2(ybuf[at, :] - top)
            expo[at, cols] = e.astype(jnp.bfloat16)
            return total + jnp.sum(e, axis=0, keepdims=True)

        total = lax.fori_loop(0, half // kb, powers, jnp.zeros((1, pb), jnp.float32), unroll=True)
        base = col // LANES
        for h in range(pb // LANES):
            stats[mine, pl.ds(base + h, 1), :] = top[:, h * LANES:(h + 1) * LANES]
            stats[mine, pl.ds(nrow + base + h, 1), :] = total[:, h * LANES:(h + 1) * LANES]

    def own(b, carry):
        block(pown, b * pb, x * rows + b * pb)
        return carry

    sends = []

    def arrived(owner, j):
        remote(
            precv.at[span(owner, j)], precv.at[span(owner, j)],
            px_send.at[0], pt_recv.at[owner * nsub + j], other, cent,
        ).wait_recv()

    def forward(owner, j, dp, ce, sem):
        copy = remote(
            precv.at[span(owner, j)], precv.at[span(owner, j)],
            sem, pt_recv.at[owner * nsub + j], dp, ce,
        )
        copy.start()
        sends.append(copy)

    ny = ncent // 2
    same = [lax.rem(yy + d, ny) * 2 + core for d in range(1, ny)]
    cross = [lax.rem(yy + d, ny) * 2 + (1 - core) for d in range(1, ny)]

    def theirs(owner, b, wait):
        if wait:
            for j in range(per):
                arrived(owner, b * per + j)
        row = owner * share + b * pb
        block(precv, row, (1 - x) * rows + row)

    nown = rows // pb
    lax.fori_loop(0, nown // 2, own, 0)
    for j in range(nsub + 1):
        if j == 1:
            lax.fori_loop(nown // 2, nown, own, 0)
        if j < nsub:
            arrived(cent, j)
            for i, d in enumerate(same):
                forward(cent, j, me, d, py_send.at[i * nsub + j])
            forward(cent, j, me, mate, pc_send.at[j])
        if j >= 1:
            for i, d in enumerate(same):
                arrived(d, j - 1)
                forward(d, j - 1, me, mate, pc_send.at[(i + 1) * nsub + j - 1])
        if j < nsub and j % per == per - 1:
            theirs(cent, j // per, False)
        if j >= 1 and (j - 1) % per == per - 1:
            theirs(mate, (j - 1) // per, True)
    for b in range(nblk):
        for d in same:
            theirs(d, b, False)
        for d in cross:
            theirs(d, b, True)

    group = 2 * ncent
    stat_sends = []
    for o in range(1, group):
        peer = lax.rem(mine + o, group)
        copy = remote(
            stats.at[mine], stats.at[mine], st_send.at[o], st_recv.at[mine],
            z * 2 + peer // ncent, lax.rem(peer, ncent),
        )
        copy.start()
        stat_sends.append(copy)
    for o in range(1, group):
        peer = lax.rem(mine + o, group)
        remote(
            stats.at[peer], stats.at[peer], st_send.at[o], st_recv.at[peer], other, cent
        ).wait_recv()
    high = stats[0, 0:nrow, :]
    for s in range(1, group):
        high = jnp.maximum(high, stats[s, 0:nrow, :])
    summed = jnp.zeros((nrow, LANES), jnp.float32)
    for s in range(group):
        summed = summed + stats[s, nrow:, :] * jnp.exp2(stats[s, 0:nrow, :] - high)
    scale_ref[...] = jnp.exp2(stats[mine, 0:nrow, :] - high) / summed

    def place(d):
        return z if d == 0 else last - z

    def ahead(d):
        return (z + 1 if d == 0 else z - 1) * 2 + x

    def behind(d):
        return (z - 1 if d == 0 else z + 1) * 2 + x

    def crows(d, i):
        return pl.ds(pl.multiple_of(d * dirs + i * chunk, chunk), chunk)

    pair = LANES // chunk
    ncnt = count // pair
    window = LAG * last

    def pass_on(d, i, src, cnt):
        remote(
            src.at[crows(d, i)], recv.at[crows(d, i)],
            rs_send.at[d], rs_recv.at[d * count + i], ahead(d), cent,
        ).start()

        @pl.when(lax.rem(i, pair) == 0)
        def _():
            slot = d * ncnt + i // pair
            remote(
                cnt.at[slot], cnt_recv.at[slot], cn_send.at[d], cn_recv.at[slot], ahead(d), cent
            ).start()

    def weigh(d, j):
        at = pl.ds(pl.multiple_of(d * dirs + j * mb, mb), mb)

        def rescale(q, acc):
            cols = pl.ds(pl.multiple_of(q * LANES, LANES), LANES)
            r = expo[at, cols].astype(jnp.float32) * scale_ref[pl.ds(q, 1), :]
            r = r.astype(jnp.bfloat16)
            expo[at, cols] = r
            return acc + r.astype(jnp.float32)

        acc = lax.fori_loop(0, nrow, rescale, jnp.zeros((mb, LANES), jnp.float32), unroll=True)
        for h in range(mb // LANES):
            line = jnp.sum(acc[h * LANES:(h + 1) * LANES, :].T, axis=0, keepdims=True)
            cnt_part[d * ncnt + j * (mb // LANES) + h] = jnp.broadcast_to(line, (8, LANES))
        part[at, :] = jnp.dot(expo[at, :], ph[...], preferred_element_type=jnp.float32)

        for which in (0, 1):
            @pl.when(jnp.logical_and(d == which, place(which) == 0))
            def _():
                for h in range(mb // chunk):
                    i = j * (mb // chunk) + h

                    @pl.when(i < window)
                    def _():
                        pass_on(which, i, part, cnt_part)

    def both(t, carry):
        first = jnp.where(z < chain // 2, 0, 1)
        d = lax.rem(first + lax.rem(t, 2), 2)
        weigh(d, t // 2)
        return carry

    def hand_out(d, i):
        rows_out = pl.ds(pl.multiple_of(x * half + d * dirs + i * chunk, chunk), chunk)
        src = final.at[crows(d, i)]
        remote(src, out_ref.at[rows_out], xp_send.at[d], xp_recv.at[d], other, cent).start()
        pltpu.make_async_copy(src, out_ref.at[rows_out], out_sem.at[d]).start()

        @pl.when(place(d) > 0)
        def _():
            remote(
                src, src, ag_send.at[d], ag_recv.at[d * count + i], behind(d), cent
            ).start()

    def tick(t, carry):
        for d in (0, 1):
            pos = place(d)
            i = t - LAG * pos

            @pl.when((pos == 0) & (i >= window) & (i < count))
            def _():
                pass_on(d, i, part, cnt_part)

            @pl.when((pos > 0) & (i >= 0) & (i < count))
            def _():
                at = crows(d, i)
                slot = d * ncnt + i // pair
                remote(
                    recv.at[at], recv.at[at], rs_send.at[d], rs_recv.at[d * count + i], other, cent
                ).wait_recv()

                @pl.when(lax.rem(i, pair) == 0)
                def _():
                    remote(
                        cnt_recv.at[slot], cnt_recv.at[slot],
                        cn_send.at[d], cn_recv.at[slot], other, cent,
                    ).wait_recv()

                @pl.when(pos < last)
                def _():
                    recv[at, :] = recv[at, :] + part[at, :]

                    @pl.when(lax.rem(i, pair) == 0)
                    def _():
                        cnt_recv[slot] = cnt_recv[slot] + cnt_part[slot]

                    pass_on(d, i, recv, cnt_recv)

                @pl.when(pos == last)
                def _():
                    @pl.when(lax.rem(i, pair) == 0)
                    def _():
                        line = cnt_recv[slot] + cnt_part[slot] + 1.0
                        cnt_col[d] = jnp.broadcast_to(line[0:1, :], (LANES, LANES)).T

                    div = cnt_col[d, pl.ds(pl.multiple_of(lax.rem(i, pair) * chunk, chunk), chunk), :]
                    div = jnp.concatenate([div] * (width // LANES), axis=1)
                    final[at, :] = (recv[at, :] + part[at, :] + cenf[at, :]) / div
                    hand_out(d, i)

        for d in (0, 1):
            pos = place(d)
            i = t - LAG * (2 * last - pos)

            @pl.when((pos < last) & (i >= 0) & (i < count))
            def _():
                at = crows(d, i)
                remote(
                    final.at[at], final.at[at], ag_send.at[d], ag_recv.at[d * count + i], other, cent
                ).wait_recv()
                hand_out(d, i)

        return carry

    units = 2 * (dirs // mb)
    early = max(2, units - window)

    def mixed(t, carry):
        tick(t, carry)
        return both(early + t, carry)

    lax.fori_loop(0, early, both, 0)
    lax.fori_loop(0, units - early, mixed, 0)
    lax.fori_loop(units - early, count + LAG * 2 * last, tick, 0)

    for copy in swaps + sends + stat_sends:
        copy.wait_send()
    for d in (0, 1):
        at = pl.ds(d * dirs, dirs)
        cs = pl.ds(d * ncnt, ncnt)

        @pl.when(place(d) < last)
        def _():
            remote(recv.at[at], recv.at[at], rs_send.at[d], rs_recv.at[0], other, cent).wait_send()
            remote(
                cnt_recv.at[cs], cnt_recv.at[cs], cn_send.at[d], cn_recv.at[0], other, cent
            ).wait_send()

        @pl.when(place(d) > 0)
        def _():
            remote(final.at[at], final.at[at], ag_send.at[d], ag_recv.at[0], other, cent).wait_send()

        here = pl.ds(pl.multiple_of(x * half + d * dirs, dirs), dirs)
        there = pl.ds(pl.multiple_of((1 - x) * half + d * dirs, dirs), dirs)
        pltpu.make_async_copy(final.at[at], out_ref.at[here], out_sem.at[d]).wait()
        remote(final.at[at], out_ref.at[there], xp_send.at[d], xp_recv.at[d], other, cent).wait()


def body(ndp, ncent, points, centroids):
    rows, width = points.shape
    half = centroids.shape[0] // 2
    share = rows // ncent
    pb = min(256, share)
    sub = pb // 4
    kb, mb, chunk = 512, 256, 32
    dirs = half // 2
    count = dirs // chunk
    ncnt = dirs // LANES
    nsub = share // sub
    ny = ncent // 2
    nrow = 2 * rows // LANES
    f32, bf16 = jnp.float32, jnp.bfloat16
    dma = pltpu.SemaphoreType.DMA
    return pl.pallas_call(
        functools.partial(kernel, ndp, ncent, (rows, half, pb, sub, kb, mb, chunk)),
        out_shape=jax.ShapeDtypeStruct(centroids.shape, f32),
        in_specs=[pl.BlockSpec(memory_space=pl.ANY)] * 2,
        out_specs=pl.BlockSpec(memory_space=pl.ANY),
        scratch_shapes=[
            pltpu.VMEM((rows, width), f32),
            pltpu.VMEM((rows, width), f32),
            pltpu.VMEM((2 * rows, width), bf16),
            pltpu.VMEM((half, width), f32),
            pltpu.VMEM((half, width), bf16),
            pltpu.VMEM((half, LANES), f32),
            pltpu.VMEM((half, pb), f32),
            pltpu.VMEM((half, 2 * rows), bf16),
            pltpu.VMEM((2 * ncent, 2 * nrow, LANES), f32),
            pltpu.VMEM((nrow, LANES), f32),
            pltpu.VMEM((half, width), f32),
            pltpu.VMEM((half, width), f32),
            pltpu.VMEM((half, width), f32),
            pltpu.VMEM((2 * ncnt, 8, LANES), f32),
            pltpu.VMEM((2 * ncnt, 8, LANES), f32),
            pltpu.VMEM((2, LANES, LANES), f32),
            dma((2,)),
            dma((ncent * nsub,)),
            dma((nsub,)),
            dma(((ny - 1) * nsub,)),
            dma((ny * nsub,)),
            dma((2 * ncent,)),
            dma((2 * ncent,)),
            dma((2,)),
            dma((2 * count,)),
            dma((2,)),
            dma((2 * ncnt,)),
            dma((2,)),
            dma((2 * count,)),
            dma((2,)),
            dma((2,)),
            dma((2,)),
        ],
        compiler_params=pltpu.CompilerParams(
            collective_id=0, has_side_effects=True, vmem_limit_bytes=63 * 2**20
        ),
        name="kmeans",
    )(points, centroids)


def solution(mesh):
    placed = (P("dp", None), P("cent", None))
    return jax.shard_map(
        functools.partial(body, mesh.shape["dp"], mesh.shape["cent"]),
        mesh=mesh, in_specs=placed, out_specs=P("cent", None), check_vma=False,
    )
```
